32 devices in a mesh: layer: 4 (over x, core), harm: 8 (over z, y).
Axes of the slice: x: 2, y: 2, z: 4, core: 2. Of those that a mesh axis runs over, the one named last changes fastest.
Arguments:
- source: bfloat16 [2, 2048, 128], P(None, 'harm'), may hold values from -6 to 6
- transfer: bfloat16 [4, 2, 2048, 2048], P('layer', None, 'harm'), may hold values from -0.09375 to 0.09375
- fields: bfloat16 [4, 2, 2048, 128], P('layer', None, 'harm'), may hold values from -6 to 6
- orders: int32 [2048], replicated, may hold values from 0 to 2047, each once
Outputs:
- gradients: float32 [4, 2, 4096], P('layer', None, 'harm')
- boundary: bfloat16 [4, 2, 2048, 128], P('layer', None, 'harm')
The draws below stay inside these ranges and needn't reach their ends.
Inputs may be any that keep to these rules, and one draw needn't show every extreme that they name: `orders`: every value from 0 to 2047 appears exactly once.
All inputs are finite; a program needn't handle non-finite values.
Results may differ from the reference program's by a relative error of at most 0.006.
Values may be sent and summed in bfloat16 or wider, within the bound.
A program may use at most 64 MiB of HBM per device.

```python
import math
import jax
import jax.numpy as jnp
from jax import lax

HARM = 2048
LAYERS_DEV = 1
BATCH = 128
LAYERS = 4
N_HARM = 8


def shard_levels(key, extent, shards, least, high):
    def one(dim, blocks):
        draws = jax.random.uniform(jax.random.fold_in(jax.random.fold_in(key, 6), dim), (blocks,), jnp.float32, least / len(shards), high / len(shards))
        return jnp.repeat(jnp.exp(draws), extent[dim] // blocks).reshape((-1,) + (1,) * (len(extent) - dim - 1))

    level = one(*shards[0])
    for cut in shards[1:]:
        level = level * one(*cut)
    return level


def normal_values(stream_key, shape, deviation, bound, cuts=(), kind=jnp.bfloat16):
    drawn = jax.random.normal(stream_key, shape, jnp.float32) * deviation
    if len(cuts) > 0:
        drawn = shard_levels(stream_key, shape, cuts, -0.22, 0.18) * drawn
    return jnp.clip(drawn, min=-bound, max=bound).astype(kind)


def setup_inputs(seed: int = 0) -> dict:
    splits = jax.random.split(jax.random.key(seed), 5)
    source = normal_values(splits[0], (2, HARM, BATCH), 1.0, 6.0, ((1, 8),))
    transfer = normal_values(splits[1], (LAYERS, 2, HARM, HARM), (2 * HARM) ** -0.5, 0.09375, ((0, 4), (2, 8)))
    fields = normal_values(splits[2], (LAYERS, 2, HARM, BATCH), 1.0, 6.0, ((0, 4), (2, 8)))
    orders = jax.random.permutation(splits[3], HARM).astype(jnp.int32)
    return dict(source=source, transfer=transfer, fields=fields, orders=orders)


def correlate(adjoint, forward, position, band_start, band_width):
    harmonics = adjoint.shape[1]
    columns = adjoint.shape[2]
    adj_sorted = jnp.take(adjoint, position, axis=1).astype(jnp.float32)
    fwd_sorted = jnp.take(forward, position, axis=1).astype(jnp.float32)
    padded = jnp.pad(adj_sorted, ((0, 0), (harmonics, harmonics + 1), (0, 0)))
    window_slab = lax.dynamic_slice_in_dim(padded, band_start + 1, harmonics + band_width, 1)
    count = harmonics // band_width
    blocks = window_slab.reshape(2, count + 1, band_width, columns)
    windows = jnp.concatenate([blocks[:, :-1], blocks[:, 1:]], axis=2)
    forward_blocks = fwd_sorted.reshape(2, count, band_width, columns)

    def product(left_part, right_part):
        return jnp.einsum('nkb,ncb->nkc', left_part, right_part)
    real_part = product(forward_blocks[0], windows[0]) - product(forward_blocks[1], windows[1])
    imag_part = product(forward_blocks[0], windows[1]) + product(forward_blocks[1], windows[0])

    def diagonals(result_block):
        flattened = result_block.reshape(count, band_width * 2 * band_width)
        flattened = jnp.pad(flattened, ((0, 0), (0, band_width)))
        shaped = flattened.reshape(count, band_width, 2 * band_width + 1)[:, :, :band_width]
        return lax.optimization_barrier(jnp.sum(shaped, axis=(0, 1)))
    return jnp.stack([diagonals(real_part), diagonals(imag_part)])

def reference(source, transfer, fields, orders):
    harmonics = orders.shape[0]
    columns = source.shape[2]
    layer_count = transfer.shape[0]
    position = jnp.zeros((harmonics,), jnp.int32).at[orders].set(jnp.arange(harmonics, dtype=jnp.int32))
    band_width = 2 * harmonics // N_HARM
    norm_scale = 1.0 / math.sqrt(harmonics * columns)
    starts = jnp.arange(0, 2 * harmonics, band_width, dtype=jnp.int32)
    adjoint = source
    grads = [None] * layer_count
    bounds = []
    for layer_index in range(layer_count - 1, -1, -1):
        forward = fields[layer_index]
        bands = lax.map(lambda band_start: correlate(adjoint, forward, position, band_start, band_width), starts)
        grads[layer_index] = jnp.transpose(bands, (1, 0, 2)).reshape(2, 2 * harmonics) * norm_scale
        matrix = transfer[layer_index]
        real_part = jnp.dot(matrix[0], adjoint[0], preferred_element_type=jnp.float32) - jnp.dot(matrix[1], adjoint[1], preferred_element_type=jnp.float32)
        imag_part = jnp.dot(matrix[0], adjoint[1], preferred_element_type=jnp.float32) + jnp.dot(matrix[1], adjoint[0], preferred_element_type=jnp.float32)
        adjoint = jnp.stack([real_part, imag_part]).astype(jnp.bfloat16)
        if layer_index % LAYERS_DEV == 0:
            bounds.append(adjoint)
    return (jnp.stack(grads), jnp.stack(bounds[::-1]))
```

```python
import contextlib
import functools
import math

import jax
import jax.numpy as jnp
from jax import lax
from jax.experimental import pallas as pl
from jax.experimental.pallas import tpu as pltpu
from jax.sharding import PartitionSpec as P

MESH = pl.DeviceIdType.MESH
REACH = 3
CHUNKS = 4


def scope(name):
    return contextlib.nullcontext()


def flipped(index, bits, count):
    total = 0
    place = 1
    while place < count:
        digit = (index // place) % 2
        total = total + (1 - digit if (bits // place) % 2 else digit) * place
        place *= 2
    return total


def across(left_values, right_values):
    return lax.dot_general(
        left_values, right_values, (((1,), (1,)), ((), ())), preferred_element_type=jnp.float32
    )


def guarded(condition, action):
    if condition is None:
        action()
    else:
        pl.when(condition)(action)


def sweep_kernel(
    sections,
    members,
    inner,
    block,
    source_ref,
    transfer_ref,
    fields_ref,
    orders_ref,
    grads_ref,
    bottom_ref,
    matrix,
    staged,
    adj,
    fwd,
    out_block,
    onehot_adj,
    onehot_fwd,
    left,
    padded,
    local_sems,
    go_sem,
    adj_recv,
    adj_send,
    adj_relay,
    adj_forward,
    down_send,
    fwd_recv,
    fwd_send,
    fwd_relay,
    fwd_forward,
):
    outer = members // inner
    section = lax.axis_index("layer")
    member = lax.axis_index("harm")
    o_index, i_index = member // inner, member % inner
    columns, rows = out_block.shape[1:]
    harmonics = members * rows
    chunks = adj_recv.shape[0]
    span = columns // chunks
    band = 2 * harmonics // members
    width = block + band
    top = section == sections - 1
    early = section < sections // 2
    from_chip = section % 2 == 0
    reach = min(REACH, outer - 1)
    near = sorted(range(1 - outer, outer), key=abs)
    order = sorted(range(-reach, reach + 1), key=abs)
    aligned = rows % 128 == 0

    def rows_of(index):
        return pl.ds(pl.multiple_of(index * rows, rows), rows)

    def sources_of(m):
        return pl.ds(m * span, span)

    load_matrix = pltpu.make_async_copy(transfer_ref.at[0], matrix, local_sems.at[0])
    load_source = pltpu.make_async_copy(source_ref, staged, local_sems.at[1])
    load_fields = [
        pltpu.make_async_copy(
            fields_ref.at[0, part], fwd.at[rows_of(member), pl.ds(part * columns, columns)], local_sems.at[2 + part]
        )
        for part in range(2)
    ]
    load_source.start()
    load_matrix.start()
    for load in load_fields:
        load.start()

    barrier = pltpu.get_barrier_semaphore()
    peers = [(section, flipped(member, t, members)) for t in range(1, members)]
    for step in (1, sections - 1):
        peers += [((section + step) % sections, flipped(member, t, members)) for t in range(members)]
    for peer in peers:
        pl.semaphore_signal(barrier, inc=1, device_id=peer, device_id_type=MESH)
    load_source.wait()

    @pl.when(top)
    def _():
        for part in range(2):
            adj[member, part] = staged[part].T

    with scope("bar"):
        pl.semaphore_wait(barrier, len(peers))

    def present(d):
        return None if d == 0 else jnp.logical_and(o_index + d >= 0, o_index + d < outer)

    def adj_view(m, held):
        return adj.at[held, :, sources_of(m), :]

    def fwd_view(m, held):
        return fwd.at[rows_of(held), :]

    def send_view(m, held):
        return out_block.at[:, sources_of(m), :]

    def line_copy(view, send, recv, m, d, u, down=False):
        return pltpu.make_async_remote_copy(
            src_ref=send_view(m, member) if down else view(m, member),
            dst_ref=view(m, member),
            send_sem=send.at[m, d + reach, u],
            recv_sem=recv.at[m, member],
            device_id=(section - 1 if down else section, (o_index + d) * inner + flipped(i_index, u, inner)),
            device_id_type=MESH,
        )

    def forward_copy(view, send, recv, m, d, u):
        held = member - d * inner
        return pltpu.make_async_remote_copy(
            src_ref=view(m, held),
            dst_ref=view(m, held),
            send_sem=send.at[m, d + outer - 1, u],
            recv_sem=recv.at[m, held],
            device_id=(section, o_index * inner + flipped(i_index, u, inner)),
            device_id_type=MESH,
        )

    def relay_copy(view, send, recv, m, d):
        held = member - d * inner
        return pltpu.make_async_remote_copy(
            src_ref=view(m, held),
            dst_ref=view(m, held),
            send_sem=send.at[m, d + outer - 1],
            recv_sem=recv.at[m, held],
            device_id=(section, member + (inner if d > 0 else -inner)),
            device_id_type=MESH,
        )

    def relays(d):
        return reach <= abs(d) < outer - 1

    def onward(d):
        step = 1 if d > 0 else -1
        return jnp.logical_and(o_index + step >= 0, o_index + step < outer)

    def arrival(view, recv, m, index):
        return pltpu.make_async_remote_copy(
            src_ref=view(m, index),
            dst_ref=view(m, index),
            send_sem=recv.at[m, index],
            recv_sem=recv.at[m, index],
            device_id=(section, index),
            device_id_type=MESH,
        )

    def each_line(view, send, recv, m, finish=False, down=False):
        for d in order:
            for u in range(inner if d == 0 else 1):
                if not down and d == 0 and u == 0:
                    continue
                copy = line_copy(view, send, recv, m, d, u, down)
                condition = present(d)
                if down and d == 0 and u > 0:
                    condition = jnp.logical_not(from_chip)
                guarded(condition, copy.wait_send if finish else copy.start)

    def each_down(m, finish=False):
        each_line(adj_view, down_send, adj_recv, m, finish, down=True)

    def pass_on(view, recv, relay, forward, m, d, finish=False, cross_here=None):
        if relays(d):
            copy = relay_copy(view, relay, recv, m, d)
            guarded(onward(d), copy.wait_send if finish else copy.start)
        if d == 0 and cross_here is None:
            return
        for u in range(1, inner):
            copy = forward_copy(view, forward, recv, m, d, u)
            guarded(cross_here if d == 0 else None, copy.wait_send if finish else copy.start)

    def collect_line(view, recv, relay, forward, m, own_here, cross_here=None):
        for d in near:

            def step(d=d):
                if d == 0 and own_here is None:
                    pass
                elif d == 0:
                    pl.when(jnp.logical_not(own_here))(arrival(view, recv, m, member).wait_recv)
                else:
                    arrival(view, recv, m, member - d * inner).wait_recv()
                pass_on(view, recv, relay, forward, m, d, cross_here=cross_here)

            guarded(present(-d), step)

    def crossed(t, u):
        return flipped(o_index, t, outer) * inner + flipped(i_index, u, inner)

    def collect_inner(view, recv, m):
        for t in range(outer):
            for u in range(1, inner):
                arrival(view, recv, m, crossed(t, u)).wait_recv()

    def finish_passing(view, recv, relay, forward, m, cross_here=None):
        for d in near:
            guarded(
                present(-d),
                functools.partial(
                    pass_on, view, recv, relay, forward, m, d, finish=True, cross_here=cross_here
                ),
            )

    def start_fields():
        for m in range(fwd_recv.shape[0]):
            each_line(fwd_view, fwd_send, fwd_recv, m)

    def relay_fields():
        for m in range(fwd_recv.shape[0]):
            collect_line(fwd_view, fwd_recv, fwd_relay, fwd_forward, m, None)

    def finish_fields():
        for m in range(fwd_recv.shape[0]):
            collect_inner(fwd_view, fwd_recv, m)

    def build_onehots():
        @pl.loop(0, harmonics // block)
        def _(index):
            start = pl.multiple_of(index * block, block)
            line = lax.broadcasted_iota(jnp.int32, (block, harmonics), 0)
            orders = orders_ref[...].reshape(1, harmonics) - start
            dtype = onehot_adj.dtype
            onehot_adj[pl.ds(start, block), :] = jnp.where(orders == line, 1.0, 0.0).astype(dtype)
            onehot_fwd[pl.ds(start, block), :] = jnp.where(orders == block - 1 - line, 1.0, 0.0).astype(dtype)

        padded[:, :harmonics] = jnp.zeros((2 * columns, harmonics), padded.dtype)
        padded[:, 2 * harmonics :] = jnp.zeros((2 * columns, harmonics), padded.dtype)

    batch = math.gcd(4, harmonics // block)

    def sort_fields():
        @pl.loop(0, harmonics // (block * batch))
        def _(index):
            start = pl.multiple_of(index * block * batch, block * batch)
            sorted_rows = jnp.dot(
                onehot_fwd[pl.ds(start, block * batch), :], fwd[...], preferred_element_type=jnp.float32
            )
            for part in range(batch):
                piece = sorted_rows[part * block : (part + 1) * block]
                real, imag = piece[:, :columns], piece[:, columns:]
                at = index * batch + part
                left[at, :block, :] = jnp.concatenate([real, -imag], axis=1).astype(left.dtype)
                left[at, block:, :] = jnp.concatenate([imag, real], axis=1).astype(left.dtype)

    tile = math.gcd(512, harmonics)

    def sort_adjoint():
        @pl.loop(0, harmonics // tile)
        def _(index):
            start = pl.multiple_of(index * tile, tile)
            total = None
            for held in range(members):
                values = adj[held].reshape(2 * columns, rows)
                term = across(values, onehot_adj[pl.ds(start, tile), held * rows : (held + 1) * rows])
                total = term if total is None else total + term
            padded[:, pl.ds(pl.multiple_of(harmonics + start, tile), tile)] = total.astype(padded.dtype)

    @pl.when(top)
    def _():
        for m in range(chunks):
            each_line(adj_view, adj_send, adj_recv, m)

    for load in load_fields:
        load.wait()

    @pl.when(jnp.logical_not(early) & jnp.logical_not(top))
    def _():
        build_onehots()

    @pl.when(section < sections // 2 - 1)
    def _():
        build_onehots()
        pl.semaphore_wait(go_sem, 1)

    @pl.when(early)
    def _():
        start_fields()

    @pl.when(section == sections // 2 - 1)
    def _():
        build_onehots()

    @pl.when(early)
    def _():
        with scope("ef_relay"):
            relay_fields()
        with scope("ef_finish"):
            finish_fields()

    @pl.when(early & (section > 0))
    def _():
        pl.semaphore_signal(go_sem, inc=1, device_id=(section - 1, member), device_id_type=MESH)

    @pl.when(early)
    def _():
        with scope("ef_sort"):
            sort_fields()

    load_matrix.wait()
    cross_adj = jnp.logical_not(from_chip) & jnp.logical_not(top)
    partials = {}

    def terms(m, helds):
        total = None
        for held in helds:
            real, imag = adj[held, 0, sources_of(m), :], adj[held, 1, sources_of(m), :]
            here = rows_of(held) if aligned else slice(held * rows, (held + 1) * rows)
            for part, values in enumerate(([real, imag], [-imag, real])):
                term = across(jnp.concatenate(values, axis=0), matrix[part, :, here])
                total = term if total is None else total + term
        return total

    def line_step(m):
        with scope("line%d" % m):
            collect_line(adj_view, adj_recv, adj_relay, adj_forward, m, top, cross_adj)

    def first_step(m):
        if aligned:
            partials[m] = terms(m, [crossed(t, 0) for t in range(outer)])

    def last_step(m):
        with scope("inner%d" % m):
            collect_inner(adj_view, adj_recv, m)
        if aligned:
            total = partials[m] + terms(m, [crossed(t, u) for t in range(outer) for u in range(1, inner)])
        else:
            total = terms(m, range(members))
        for part in range(2):
            out_block[part, sources_of(m), :] = total[part * span : (part + 1) * span].astype(out_block.dtype)

        @pl.when(section > 0)
        def _():
            each_down(m)

    ahead = 2
    for m in range(chunks + ahead):
        if m < chunks:
            line_step(m)
        if m >= ahead:
            last_step(m - ahead)
        if m < chunks:
            first_step(m)

    for part in range(2):
        bottom_ref[part] = out_block[part].T

    @pl.when(top)
    def _():
        build_onehots()

    @pl.when(jnp.logical_not(early))
    def _():
        with scope("lf_relay"):
            start_fields()
            relay_fields()
        with scope("lsortadj"):
            sort_adjoint()
        with scope("lf_finish"):
            finish_fields()
        with scope("lf_sort"):
            sort_fields()

    @pl.when(early)
    def _():
        with scope("esortadj"):
            sort_adjoint()

    with scope("grad"):
        total = jnp.zeros((2 * block, width), jnp.float32)
        for index in range(harmonics // block):
            start = member * band + index * block
            if block % 128 == 0:
                window = padded[:, pl.ds(pl.multiple_of(start, block), width)]
            else:
                near_start = pl.multiple_of(start // 128 * 128, 128)
                wide = padded[:, pl.ds(near_start, (width + 255) // 128 * 128)]
                window = wide[:, :width]
                for shift in range(block, 128, block):
                    window = jnp.where(start - near_start == shift, wide[:, shift : shift + width], window)
            total = total + jnp.dot(left[index], window, preferred_element_type=jnp.float32)
        for part in range(2):
            rolled = pltpu.roll(
                total[part * block : (part + 1) * block], width - block, 1, stride=1, stride_axis=0
            )
            grads_ref[part : part + 1, :] = jnp.sum(rolled, axis=0, keepdims=True)[:, :band]

    with scope("fin"):
        for m in range(chunks):
            finish_passing(adj_view, adj_recv, adj_relay, adj_forward, m, cross_adj)
        for m in range(fwd_recv.shape[0]):
            each_line(fwd_view, fwd_send, fwd_recv, m, finish=True)
            finish_passing(fwd_view, fwd_recv, fwd_relay, fwd_forward, m)

        @pl.when(top)
        def _():
            for m in range(chunks):
                each_line(adj_view, adj_send, adj_recv, m, finish=True)

        @pl.when(section > 0)
        def _():
            for m in range(chunks):
                each_down(m, finish=True)


def per_device(source, transfer, fields, orders):
    harmonics = orders.shape[0]
    sections = lax.axis_size("layer")
    members = lax.axis_size("harm")
    rows = transfer.shape[2]
    columns = source.shape[2]
    inner = 1 << ((members.bit_length() - 1) // 2)
    outer = members // inner
    band = 2 * harmonics // members
    block = min(128, band)
    chunks = math.gcd(CHUNKS, columns)
    reach = min(REACH, outer - 1)
    norm_scale = 1.0 / math.sqrt(harmonics * columns)
    any_space = pl.BlockSpec(memory_space=pl.ANY)
    vmem = pl.BlockSpec(memory_space=pltpu.VMEM)
    dma = pltpu.SemaphoreType.DMA
    grads, bottom = pl.pallas_call(
        functools.partial(sweep_kernel, sections, members, inner, block),
        out_shape=(
            jax.ShapeDtypeStruct((2, band), jnp.float32),
            jax.ShapeDtypeStruct((2, rows, columns), jnp.bfloat16),
        ),
        in_specs=[any_space, any_space, any_space, vmem],
        out_specs=(vmem, vmem),
        scratch_shapes=[
            pltpu.VMEM((2, rows, harmonics), jnp.bfloat16),
            pltpu.VMEM((2, rows, columns), jnp.bfloat16),
            pltpu.VMEM((members, 2, columns, rows), jnp.bfloat16),
            pltpu.VMEM((harmonics, 2 * columns), jnp.bfloat16),
            pltpu.VMEM((2, columns, rows), jnp.bfloat16),
            pltpu.VMEM((harmonics, harmonics), jnp.bfloat16),
            pltpu.VMEM((harmonics, harmonics), jnp.bfloat16),
            pltpu.VMEM((harmonics // block, 2 * block, 2 * columns), jnp.bfloat16),
            pltpu.VMEM((2 * columns, 3 * harmonics), jnp.bfloat16),
            dma((4,)),
            pltpu.SemaphoreType.REGULAR,
            dma((chunks, members)),
            dma((chunks, 2 * reach + 1, inner)),
            dma((chunks, 2 * outer - 1)),
            dma((chunks, 2 * outer - 1, inner)),
            dma((chunks, 2 * reach + 1, inner)),
            dma((1, members)),
            dma((1, 2 * reach + 1, inner)),
            dma((1, 2 * outer - 1)),
            dma((1, 2 * outer - 1, inner)),
        ],
        compiler_params=pltpu.CompilerParams(collective_id=0, has_side_effects=True),
        name="sweep",
    )(source, transfer, fields, orders)
    return (grads * norm_scale)[None], bottom[None]


def solution(mesh):
    return jax.shard_map(
        per_device,
        mesh=mesh,
        in_specs=(
            P(None, "harm", None),
            P("layer", None, "harm", None),
            P("layer", None, "harm", None),
            P(),
        ),
        out_specs=(P("layer", None, "harm"), P("layer", None, "harm", None)),
        check_vma=False,
    )
```

```python
import contextlib
import functools
import math

import jax
import jax.numpy as jnp
from jax import lax
from jax.experimental import pallas as pl
from jax.experimental.pallas import tpu as pltpu
from jax.sharding import PartitionSpec as P

MESH = pl.DeviceIdType.MESH
CHUNKS = 4
AHEAD = 2


def scope(name):
    return contextlib.nullcontext()


def flipped(index, bits, count):
    total = 0
    place = 1
    while place < count:
        digit = (index // place) % 2
        total = total + (1 - digit if (bits // place) % 2 else digit) * place
        place *= 2
    return total


def guarded(condition, action):
    if condition is None:
        action()
    else:
        pl.when(condition)(action)


def sweep_kernel(
    sections,
    members,
    inner,
    block,
    source_ref,
    transfer_ref,
    fields_ref,
    orders_ref,
    grads_ref,
    bottom_ref,
    matrix,
    turned,
    staged,
    adj,
    fwd,
    out_block,
    bottom,
    onehot_adj,
    onehot_fwd,
    left,
    padded,
    product,
    partial,
    arrived,
    local_sems,
    adj_recv,
    adj_send,
    adj_forward,
    down_send,
    fwd_recv,
    fwd_send,
    fwd_forward,
    sum_recv,
    sum_send,
):
    outer = members // inner
    section = lax.axis_index("layer")
    member = lax.axis_index("harm")
    o_index, i_index = member // inner, member % inner
    columns, rows = out_block.shape[1:]
    harmonics = members * rows
    chunks = adj_recv.shape[0]
    span = columns // chunks
    band = 2 * harmonics // members
    width = block + band
    top = section == sections - 1
    early = section < sections // 2
    crosses = section % 2 == 0

    def rows_of(index):
        return pl.ds(pl.multiple_of(index * rows, rows), rows)

    def sources_of(m):
        return pl.ds(m * span, span)

    def at(t, u):
        return flipped(o_index, t, outer) * inner + flipped(i_index, u, inner)

    load_matrix = pltpu.make_async_copy(transfer_ref.at[0], matrix, local_sems.at[0])
    load_source = pltpu.make_async_copy(source_ref, staged, local_sems.at[1])
    load_fields = [
        pltpu.make_async_copy(
            fields_ref.at[0, part], fwd.at[rows_of(member), pl.ds(part * columns, columns)], local_sems.at[2 + part]
        )
        for part in range(2)
    ]
    store_bottom = pltpu.make_async_copy(bottom, bottom_ref, local_sems.at[4])
    load_source.start()
    load_matrix.start()
    for load in load_fields:
        load.start()

    barrier = pltpu.get_barrier_semaphore()
    peers = [(section, flipped(member, t, members)) for t in range(1, members)]
    for step in (1, sections - 1):
        peers += [((section + step) % sections, flipped(member, t, members)) for t in range(members)]
    for peer in peers:
        pl.semaphore_signal(barrier, inc=1, device_id=peer, device_id_type=MESH)
    load_source.wait()

    @pl.when(top)
    def _():
        for part in range(2):
            adj[member, part] = staged[part].T

    with scope("bar"):
        pl.semaphore_wait(barrier, len(peers))

    def remote(src, dst, send_sem, recv_sem, to_section, to_member):
        return pltpu.make_async_remote_copy(
            src_ref=src,
            dst_ref=dst,
            send_sem=send_sem,
            recv_sem=recv_sem,
            device_id=(to_section, to_member),
            device_id_type=MESH,
        )

    def adj_view(m, held):
        return adj.at[held, :, sources_of(m), :]

    def fwd_view(m, held):
        return fwd.at[rows_of(held), :]

    def send_line(view, send, recv, m, finish=False, down=False):
        src = out_block.at[:, sources_of(m), :] if down else view(m, member)
        for t in range(outer):
            for u in range(inner if t == 0 else 1):
                if t == 0 and u == 0 and not down:
                    continue
                copy = remote(
                    src, view(m, member), send.at[m, t, u], recv.at[m, member], section - 1 if down else section, at(t, u)
                )
                condition = jnp.logical_not(crosses) if down and t == 0 and u > 0 else None
                guarded(condition, copy.wait_send if finish else copy.start)

    def arrival(view, recv, m, index):
        return remote(view(m, index), view(m, index), recv.at[m, index], recv.at[m, index], section, index)

    def forward(view, send, recv, m, t, finish=False):
        held = at(t, 0)
        for u in range(1, inner):
            copy = remote(view(m, held), view(m, held), send.at[m, t, u], recv.at[m, held], section, at(0, u))
            if finish:
                copy.wait_send()
            else:
                copy.start()

    def collect_line(view, send, recv, m, own_arrives=None, own_forward=None):
        if own_arrives is not None:
            pl.when(own_arrives)(arrival(view, recv, m, member).wait_recv)
        if own_forward is not None:
            pl.when(own_forward)(functools.partial(forward, view, send, recv, m, 0))
        for t in range(1, outer):
            arrival(view, recv, m, at(t, 0)).wait_recv()
            forward(view, send, recv, m, t)

    def finish_line(view, send, recv, m, own_forward=None):
        if own_forward is not None:
            pl.when(own_forward)(functools.partial(forward, view, send, recv, m, 0, finish=True))
        for t in range(1, outer):
            forward(view, send, recv, m, t, finish=True)

    def collect_inner(view, recv, m):
        for t in range(outer):
            for u in range(1, inner):
                arrival(view, recv, m, at(t, u)).wait_recv()

    lanes = min(128, harmonics)

    def build_onehots(whole):
        @pl.loop(0, harmonics // lanes)
        def _(index):
            start = pl.multiple_of(index * lanes, lanes)
            orders = orders_ref[...].reshape(1, harmonics)
            line = lax.broadcasted_iota(jnp.int32, (lanes, harmonics), 0)
            wanted = jnp.where(orders == start + line, 1.0, 0.0).astype(onehot_adj.dtype)
            onehot_adj[:, pl.ds(start, lanes)] = wanted.T

        @pl.loop(0, harmonics // block)
        def _(index):
            start = pl.multiple_of(index * block, block)
            orders = orders_ref[...].reshape(1, harmonics) - start
            if not whole:
                mine = orders[:, :rows]
                for m in range(1, members):
                    mine = jnp.where(member == m, orders[:, m * rows : (m + 1) * rows], mine)
                orders = mine
            size = orders.shape[1]
            line = lax.broadcasted_iota(jnp.int32, (block, size), 0)
            wanted = jnp.where(orders == block - 1 - line, 1.0, 0.0)
            onehot_fwd[pl.ds(start, block), :size] = wanted.astype(onehot_fwd.dtype)

        padded[:, :harmonics] = jnp.zeros((2 * columns, harmonics), padded.dtype)
        padded[:, 2 * harmonics :] = jnp.zeros((2 * columns, harmonics), padded.dtype)

    batch = math.gcd(4, harmonics // block)

    def sort_fields(whole):
        @pl.loop(0, harmonics // (block * batch))
        def _(index):
            here = pl.ds(pl.multiple_of(index * block * batch, block * batch), block * batch)
            if whole:
                sorted_rows = jnp.dot(onehot_fwd[here, :], fwd[...], preferred_element_type=jnp.float32)
            else:
                sorted_rows = jnp.dot(
                    onehot_fwd[here, :rows], fwd[rows_of(member), :], preferred_element_type=jnp.float32
                )
            for part in range(batch):
                piece = sorted_rows[part * block : (part + 1) * block]
                real, imag = piece[:, :columns], piece[:, columns:]
                place = index * batch + part
                left[place, :block, :] = jnp.concatenate([real, -imag], axis=1).astype(left.dtype)
                left[place, block:, :] = jnp.concatenate([imag, real], axis=1).astype(left.dtype)

    tile = math.gcd(512, harmonics)

    def sort_adjoint(helds, first):
        @pl.loop(0, harmonics // tile)
        def _(index):
            start = pl.multiple_of(index * tile, tile)
            here = pl.ds(pl.multiple_of(harmonics + start, tile), tile)
            total = None if first else padded[:, here].astype(jnp.float32)
            for held in helds:
                term = jnp.dot(
                    adj[held].reshape(2 * columns, rows),
                    onehot_adj[rows_of(held), pl.ds(start, tile)],
                    preferred_element_type=jnp.float32,
                )
                total = term if total is None else total + term
            padded[:, here] = total.astype(padded.dtype)

    def turn_matrix():
        deep = math.gcd(256, harmonics)

        @pl.loop(0, harmonics // deep)
        def _(index):
            here = pl.ds(pl.multiple_of(index * deep, deep), deep)
            for part in range(2):
                turned[part, here, :] = matrix[part, :, here].T

    @pl.when(top)
    def _():
        for m in range(chunks):
            send_line(adj_view, adj_send, adj_recv, m)

    for load in load_fields:
        load.wait()

    @pl.when(early)
    def _():
        send_line(fwd_view, fwd_send, fwd_recv, 0)

    load_matrix.wait()
    with scope("turn"):
        turn_matrix()

    def finish_fields():
        with scope("ef_finish"):
            collect_inner(fwd_view, fwd_recv, 0)
        with scope("ef_sort"):
            sort_fields(True)

    @pl.when(early)
    def _():
        with scope("ef_relay"):
            collect_line(fwd_view, fwd_forward, fwd_recv, 0)
        with scope("e_onehot"):
            build_onehots(True)

    @pl.when(section == 0)
    def _():
        finish_fields()

    @pl.when(jnp.logical_not(early) & jnp.logical_not(top))
    def _():
        with scope("l_onehot"):
            build_onehots(False)
        with scope("lf_sort"):
            sort_fields(False)

    own_forward = jnp.logical_not(crosses) & jnp.logical_not(top)
    near_blocks = [at(t, 0) for t in range(outer)]
    far_blocks = [at(t, u) for t in range(outer) for u in range(1, inner)]
    partials = {}

    def terms(m, helds):
        total = None
        for held in helds:
            real, imag = adj[held, 0, sources_of(m), :], adj[held, 1, sources_of(m), :]
            for part, values in enumerate(([real, imag], [-imag, real])):
                term = jnp.dot(
                    jnp.concatenate(values, axis=0),
                    turned[part, rows_of(held), :],
                    preferred_element_type=jnp.float32,
                )
                total = term if total is None else total + term
        return total

    def line_step(m):
        with scope("line%d" % m):
            collect_line(adj_view, adj_forward, adj_recv, m, jnp.logical_not(top), own_forward)

    def last_step(m):
        with scope("inner%d" % m):
            collect_inner(adj_view, adj_recv, m)
        total = partials[m] + terms(m, far_blocks)
        for part in range(2):
            out_block[part, sources_of(m), :] = total[part * span : (part + 1) * span].astype(out_block.dtype)

        @pl.when(section > 0)
        def _():
            send_line(adj_view, down_send, adj_recv, m, down=True)

    for m in range(chunks + AHEAD):
        if m < chunks:
            line_step(m)
        if m == chunks + AHEAD - 1:

            @pl.when(section == 0)
            def _():
                with scope("sort_near0"):
                    sort_adjoint(near_blocks, True)

        if m >= AHEAD:
            last_step(m - AHEAD)
        if m < chunks:
            partials[m] = terms(m, near_blocks)

    for part in range(2):
        bottom[part] = out_block[part].T
    store_bottom.start()

    @pl.when(top)
    def _():
        with scope("t_onehot"):
            build_onehots(False)
        with scope("t_sort"):
            sort_fields(False)

    @pl.when(early & (section > 0))
    def _():
        finish_fields()

    @pl.when(section > 0)
    def _():
        with scope("sort_near"):
            sort_adjoint(near_blocks, True)

    with scope("sort_far"):
        sort_adjoint(far_blocks, False)

    def diagonals(values, part):
        rolled = pltpu.roll(values[part * block : (part + 1) * block], width - block, 1, stride=1, stride_axis=0)
        return jnp.sum(rolled, axis=0, keepdims=True)[:, :band]

    @pl.when(early)
    def _():
        with scope("grad"):
            total = jnp.zeros((2 * block, width), jnp.float32)
            for index in range(harmonics // block):
                start = member * band + index * block
                if block % 128 == 0:
                    window = padded[:, pl.ds(pl.multiple_of(start, block), width)]
                else:
                    near_start = pl.multiple_of(start // 128 * 128, 128)
                    wide = padded[:, pl.ds(near_start, (width + 255) // 128 * 128)]
                    window = wide[:, :width]
                    for shift in range(block, 128, block):
                        window = jnp.where(start - near_start == shift, wide[:, shift : shift + width], window)
                total = total + jnp.dot(left[index], window, preferred_element_type=jnp.float32)
            for part in range(2):
                grads_ref[part : part + 1, :] = diagonals(total, part)

    step = math.gcd(256, 2 * harmonics)

    @pl.when(jnp.logical_not(early))
    def _():
        with scope("l_grad"):
            product[:, :block] = jnp.zeros((2 * block, block), jnp.float32)
            for first in range(0, 2 * harmonics, step):
                total = jnp.zeros((2 * block, step), jnp.float32)
                for index in range(harmonics // block):
                    start = first + block * (index + 1) - harmonics
                    if start + step > 0 and start < harmonics:
                        window = padded[:, harmonics + start : harmonics + start + step]
                        total = total + jnp.dot(left[index], window, preferred_element_type=jnp.float32)
                product[:, block + first : block + first + step] = total
        with scope("l_diag"):
            for m in range(members):
                values = product[:, m * band : m * band + width]
                for part in range(2):
                    partial[m, part : part + 1, :] = diagonals(values, part)

        def sums(t):
            to = flipped(member, t, members)
            return remote(partial.at[to], arrived.at[member], sum_send.at[t], sum_recv.at[member], section, to)

        with scope("l_sum"):
            for t in range(1, members):
                sums(t).start()
            total = partial[member]
            for t in range(1, members):
                other = flipped(member, t, members)
                remote(
                    arrived.at[other], arrived.at[other], sum_recv.at[other], sum_recv.at[other], section, other
                ).wait_recv()
                total = total + arrived[other]
            grads_ref[...] = total
            for t in range(1, members):
                sums(t).wait_send()

    with scope("fin"):
        store_bottom.wait()
        for m in range(chunks):
            finish_line(adj_view, adj_forward, adj_recv, m, own_forward)

        @pl.when(early)
        def _():
            send_line(fwd_view, fwd_send, fwd_recv, 0, finish=True)
            finish_line(fwd_view, fwd_forward, fwd_recv, 0)

        @pl.when(top)
        def _():
            for m in range(chunks):
                send_line(adj_view, adj_send, adj_recv, m, finish=True)

        @pl.when(section > 0)
        def _():
            for m in range(chunks):
                send_line(adj_view, down_send, adj_recv, m, finish=True, down=True)


def per_device(source, transfer, fields, orders):
    harmonics = orders.shape[0]
    sections = lax.axis_size("layer")
    members = lax.axis_size("harm")
    rows = transfer.shape[2]
    columns = source.shape[2]
    inner = 1 << ((members.bit_length() - 1) // 2)
    outer = members // inner
    band = 2 * harmonics // members
    block = min(128, band)
    chunks = math.gcd(CHUNKS, columns)
    norm_scale = 1.0 / math.sqrt(harmonics * columns)
    any_space = pl.BlockSpec(memory_space=pl.ANY)
    vmem = pl.BlockSpec(memory_space=pltpu.VMEM)
    dma = pltpu.SemaphoreType.DMA
    grads, bottom = pl.pallas_call(
        functools.partial(sweep_kernel, sections, members, inner, block),
        out_shape=(
            jax.ShapeDtypeStruct((2, band), jnp.float32),
            jax.ShapeDtypeStruct((2, rows, columns), jnp.bfloat16),
        ),
        in_specs=[any_space, any_space, any_space, vmem],
        out_specs=(vmem, any_space),
        scratch_shapes=[
            pltpu.VMEM((2, rows, harmonics), jnp.bfloat16),
            pltpu.VMEM((2, harmonics, rows), jnp.bfloat16),
            pltpu.VMEM((2, rows, columns), jnp.bfloat16),
            pltpu.VMEM((members, 2, columns, rows), jnp.bfloat16),
            pltpu.VMEM((harmonics, 2 * columns), jnp.bfloat16),
            pltpu.VMEM((2, columns, rows), jnp.bfloat16),
            pltpu.VMEM((2, rows, columns), jnp.bfloat16),
            pltpu.VMEM((harmonics, harmonics), jnp.bfloat16),
            pltpu.VMEM((harmonics, harmonics), jnp.bfloat16),
            pltpu.VMEM((harmonics // block, 2 * block, 2 * columns), jnp.bfloat16),
            pltpu.VMEM((2 * columns, 3 * harmonics), jnp.bfloat16),
            pltpu.VMEM((2 * block, block + 2 * harmonics), jnp.float32),
            pltpu.VMEM((members, 2, band), jnp.float32),
            pltpu.VMEM((members, 2, band), jnp.float32),
            dma((5,)),
            dma((chunks, members)),
            dma((chunks, outer, inner)),
            dma((chunks, outer, inner)),
            dma((chunks, outer, inner)),
            dma((1, members)),
            dma((1, outer, inner)),
            dma((1, outer, inner)),
            dma((members,)),
            dma((members,)),
        ],
        compiler_params=pltpu.CompilerParams(collective_id=0, has_side_effects=True),
        name="sweep",
    )(source, transfer, fields, orders)
    return (grads * norm_scale)[None], bottom[None]


def solution(mesh):
    return jax.shard_map(
        per_device,
        mesh=mesh,
        in_specs=(
            P(None, "harm", None),
            P("layer", None, "harm", None),
            P("layer", None, "harm", None),
            P(),
        ),
        out_specs=(P("layer", None, "harm"), P("layer", None, "harm", None)),
        check_vma=False,
    )
```
